128 devices in a mesh: dp: 32 (over x, z, core), mp: 4 (over y).
Axes of the slice: x: 4, y: 4, z: 4, core: 2. Of those that a mesh axis runs over, the one named last changes fastest.
Arguments:
- acts: bfloat16 [1, 65536, 4096], P(None, 'dp'), may hold values from -64 to 64
- out_grads: bfloat16 [1, 65536, 4096], P(None, 'dp', 'mp'), may hold values from -80 to 80
- clip_bound: float32 [1], replicated, may hold values from 163840 to 491520
- noise: float32 [1, 4096, 4096], P(None, 'dp', 'mp'), may hold values from -6 to 6
Outputs:
- update: float32 [1, 4096, 4096], P(None, 'dp', 'mp')
The draws below stay inside these ranges and needn't reach their ends.
All inputs are finite; a program needn't handle non-finite values.
Results may differ from the reference program's by a relative error of at most 0.0017.
Values may be sent and summed in bfloat16 or wider, within the bound.
A program may use at most 128 MiB of HBM per device.

```python
import math
import jax
import jax.numpy as jnp
from jax import lax

D = 4096
GROUPS = 1
SEQ = 512
BATCH = 128
TOKENS = 65536


def token_signs(key):
    sign_key = jax.random.fold_in(key, 37)
    flips = jax.random.bernoulli(sign_key, 0.5, (GROUPS, BATCH, SEQ, 1))
    return jnp.where(flips, 1.0, -1.0).astype(jnp.float32)


def draw_acts(key, part):
    base_key = jax.random.fold_in(key, 11)
    key_rows, key_cols, key_base = jax.random.split(base_key, 3)
    key_direction = jax.random.fold_in(base_key, 5)
    row_scale = jnp.exp(jax.random.uniform(key_rows, (GROUPS, TOKENS, 1), jnp.float32, math.log(0.3), math.log(3.0)))
    col_scale = jnp.exp(jax.random.uniform(key_cols, (GROUPS, 1, D), jnp.float32, math.log(0.3), math.log(3.0)))
    direction = jnp.clip(jax.random.normal(key_direction, (GROUPS, BATCH, 1, D), jnp.float32), -2.5, 2.5)
    shared = (0.35 * token_signs(key) * direction).reshape(GROUPS, TOKENS, D)
    base_draw = jnp.clip(jax.random.normal(key_base, (GROUPS, TOKENS, D), jnp.float32), -6.0, 6.0)
    return ((base_draw + shared) * row_scale * col_scale).astype(jnp.bfloat16)


def draw_out_grads(key, part):
    base_key = jax.random.fold_in(key, 23)
    key_examples, key_rows, key_cols, key_base = jax.random.split(base_key, 4)
    key_direction = jax.random.fold_in(base_key, 7)
    example_scale = jnp.exp(jax.random.uniform(key_examples, (GROUPS, BATCH, 1, 1), jnp.float32, math.log(0.3), math.log(3.0)))
    row_scale = jnp.exp(jax.random.uniform(key_rows, (GROUPS, BATCH, SEQ, 1), jnp.float32, math.log(0.5), math.log(2.0)))
    col_scale = jnp.exp(jax.random.uniform(key_cols, (GROUPS, 1, 1, D), jnp.float32, math.log(0.5), math.log(2.0)))
    direction = jnp.clip(jax.random.normal(key_direction, (GROUPS, BATCH, 1, D), jnp.float32), -2.5, 2.5)
    shared = 0.25 * token_signs(key) * direction
    base_draw = jnp.clip(jax.random.normal(key_base, (GROUPS, BATCH, SEQ, D), jnp.float32), -6.0, 6.0)
    values = (base_draw + shared) * example_scale * row_scale * col_scale
    return values.reshape(GROUPS, TOKENS, D).astype(jnp.bfloat16)


def block_scale(rng, dims, cuts, smallest, largest):
    factor_of = 1.0
    for position, blocks in cuts:
        heights = jax.random.uniform(jax.random.fold_in(jax.random.fold_in(rng, 6), position), (blocks,), jnp.float32, smallest / len(cuts), largest / len(cuts))
        factor_of = factor_of * jnp.repeat(jnp.exp(heights), dims[position] // blocks).reshape((-1,) + (1,) * (len(dims) - 1 - position))
    return factor_of


def bell_draw(rng, shape, spread, reach, pieces=(), held_as=jnp.bfloat16):
    values = spread * jax.random.normal(rng, shape, jnp.float32)
    if pieces:
        values = values * block_scale(rng, shape, pieces, -0.22, 0.18)
    return jnp.clip(values, -reach, reach).astype(held_as)


def setup_inputs(seed: int = 0) -> dict:
    key_of = jax.random.split(jax.random.key(seed), 5)
    acts = draw_acts(jax.random.fold_in(key_of[4], 71), 0)
    out_grads = draw_out_grads(jax.random.fold_in(key_of[4], 71), 0)
    clip_bound = jnp.clip(jnp.exp(jax.random.uniform(key_of[2], (GROUPS,), jnp.float32, math.log(163840.0), math.log(491520.0))), 163840.0, 491520.0)
    noise = bell_draw(key_of[3], (GROUPS, D, D), 0.5, 6.0, ((1, 32), (2, 4)), jnp.float32)
    return {"acts": acts, "out_grads": out_grads, "clip_bound": clip_bound, "noise": noise}


def reference(acts, out_grads, clip_bound, noise):
    results = []
    for group_index in range(GROUPS):
        act_seq = acts[group_index].reshape(BATCH, SEQ, D)
        grad_seq = out_grads[group_index].reshape(BATCH, SEQ, D)

        def one_example(pair):
            act_one, grad_one = pair
            gram_act = jnp.dot(act_one, act_one.T, preferred_element_type=jnp.float32)
            gram_grad = jnp.dot(grad_one, grad_one.T, preferred_element_type=jnp.float32)
            return jnp.sum(gram_act * gram_grad)
        norm_sq = lax.map(one_example, (act_seq, grad_seq))
        bound = clip_bound[group_index]
        clip = jnp.minimum(1.0, bound / jnp.sqrt(norm_sq + 1e-06))
        factor = clip / bound
        scaled = (grad_seq.astype(jnp.float32) * factor[:, None, None]).astype(jnp.bfloat16)
        scaled = scaled.reshape(TOKENS, D)
        summed = jnp.dot(acts[group_index].T, scaled, preferred_element_type=jnp.float32)
        results.append(summed * (D / math.sqrt(BATCH)) + noise[group_index])
    return jnp.stack(results)
```

```python
import math

import jax
import jax.numpy as jnp
from jax import lax
from jax.experimental import pallas as pl
from jax.experimental.pallas import tpu as pltpu
from jax.sharding import PartitionSpec as P

SEQ = 512
RING = 4
MESH = pl.DeviceIdType.MESH
F32 = jnp.float32
BF16 = jnp.bfloat16
CONTRACT_LAST = (((1,), (1,)), ((), ()))


def fold(product):
    rows, cols = product.shape
    return jnp.sum(product.reshape(rows // 8, 8, cols // 128, 128), axis=(0, 2))


def kernel(acts, grads, bound, out, abuf, graw, acts_c, g_t, norm_own, norm_all,
           s_opp, s_nb, hold, r_opp, r_fin, own, r2_opp, s2, r2_fin,
           abuf_sem, grad_sem, col_sem, xs_acts, xr_acts, xs_grads, xr_grads, ns_sem, nr_sem,
           s1_opp, r1_opp, s1_fin, r1_fin, s2_opp, r2o_sem, s2_fin, r2f_sem):
    dp = lax.axis_index("dp")
    y = lax.axis_index("mp")
    x, z, c = dp // (2 * RING), (dp // 2) % RING, dp % 2
    tokens = acts.shape[0]
    examples = tokens // SEQ
    blocks = acts.shape[1] // 256
    half_cols = grads.shape[1] // 2

    def at(xx, zz, cc=c, yy=y):
        return ((xx % RING) * (2 * RING) + (zz % RING) * 2 + cc, yy)

    partner = at(x, z, 1 - c)
    prim = (x, z)
    seco = (z, x)

    def hop(axis, direction):
        step = 1 if direction == 0 else RING - 1
        return at(x + step, z) if axis == 0 else at(x, z + step)

    def load_acts(e, slot):
        return pltpu.make_async_copy(acts.at[pl.ds(e * SEQ, SEQ), :], abuf.at[slot], abuf_sem.at[slot])

    def load_grads(e):
        rows = pl.ds(e * SEQ, SEQ)
        return pltpu.make_async_copy(grads.at[rows, :], graw.at[c, rows, :], grad_sem.at[e])

    load_acts(0, 0).start()
    load_grads(0).start()
    load_acts(1, 1).start()
    for e in range(1, examples):
        load_grads(e).start()

    peers = [hop(a, d) for a in (0, 1) for d in (0, 1)]
    me8 = c * 4 + y
    group = []
    for d in range(1, 8):
        other = (me8 + d) % 8
        group.append((other, at(x, z, other // 4, other % 4)))
    barrier = pltpu.get_barrier_semaphore()
    for device in peers + [g[1] for g in group]:
        pl.semaphore_signal(barrier, inc=1, device_id=device, device_id_type=MESH)
    pl.semaphore_wait(barrier, 11)

    mine = pl.ds(pl.multiple_of(c * tokens, tokens), tokens)
    send_grads = pltpu.make_async_remote_copy(
        src_ref=grads, dst_ref=graw.at[c], send_sem=xs_grads, recv_sem=xr_grads,
        device_id=partner, device_id_type=MESH)
    send_grads.start()

    def column_block(j, core):
        return pl.ds(pl.multiple_of(j * 256 + core * 128, 128), 128)

    def send_column(j):
        return pltpu.make_async_remote_copy(
            src_ref=acts.at[:, column_block(j, 1 - c)], dst_ref=acts_c.at[j, mine, :],
            send_sem=xs_acts.at[j], recv_sem=xr_acts.at[j], device_id=partner, device_id_type=MESH)

    def load_column(j):
        return pltpu.make_async_copy(acts.at[:, column_block(j, c)], acts_c.at[j, mine, :], col_sem.at[j])

    for j in range(blocks):
        send_column(j).start()
    for j in range(blocks):
        load_column(j).start()

    for e in range(examples):
        slot = e % 2
        load_acts(e, slot).wait()
        load_grads(e).wait()
        low, high = pl.ds(0, 256), pl.ds(256, 256)
        a_all = abuf[slot]
        b_rows = pl.ds(e * SEQ, SEQ)
        b_all = graw[c, b_rows, :]
        b_low = graw[c, pl.ds(e * SEQ, 256), :]
        b_high = graw[c, pl.ds(e * SEQ + 256, 256), :]
        ga = lax.dot_general(a_all, abuf[slot, low, :], CONTRACT_LAST, preferred_element_type=F32)
        gb = lax.dot_general(b_all, b_low, CONTRACT_LAST, preferred_element_type=F32)
        both = ga * gb
        total = fold(both[:256]) + 2.0 * fold(both[256:])
        a_high = abuf[slot, high, :]
        ga = lax.dot_general(a_high, a_high, CONTRACT_LAST, preferred_element_type=F32)
        gb = lax.dot_general(b_high, b_high, CONTRACT_LAST, preferred_element_type=F32)
        norm_own[e] = total + fold(ga * gb)
        if e + 2 < examples:
            load_acts(e + 2, slot).start()
        columns = pl.ds(pl.multiple_of(c * tokens + e * SEQ, SEQ), SEQ)
        g_t[:, columns] = b_all.T

    def send_norms(other, device):
        return pltpu.make_async_remote_copy(
            src_ref=norm_own, dst_ref=norm_all.at[me8], send_sem=ns_sem.at[other],
            recv_sem=nr_sem.at[me8], device_id=device, device_id_type=MESH)

    for other, device in group:
        send_norms(other, device).start()

    send_grads.wait_recv()
    theirs = 1 - c
    for e in range(examples):
        columns = pl.ds(pl.multiple_of(theirs * tokens + e * SEQ, SEQ), SEQ)
        g_t[:, columns] = graw[theirs, pl.ds(e * SEQ, SEQ), :].T

    norm_all[me8] = norm_own[...]
    for other, device in group:
        pltpu.make_async_remote_copy(
            src_ref=norm_own, dst_ref=norm_all.at[other], send_sem=ns_sem.at[other],
            recv_sem=nr_sem.at[other], device_id=device, device_id_type=MESH).wait_recv()

    limit = bound[0]
    factors = []
    for core in range(2):
        summed = norm_all[4 * core] + norm_all[4 * core + 1] + norm_all[4 * core + 2] + norm_all[4 * core + 3]
        for e in range(examples):
            norm_sq = jnp.sum(summed[e], axis=(0, 1), keepdims=True)
            clip = jnp.minimum(1.0, limit / jnp.sqrt(norm_sq + 1e-06))
            factors.append(clip / limit)

    def scale(a):
        for e, factor in enumerate(factors):
            rows, columns = pl.ds(a * half_cols, half_cols), pl.ds(e * SEQ, SEQ)
            g_t[rows, columns] = (g_t[rows, columns].astype(F32) * factor).astype(BF16)

    roles = (2, 1, 3, 0)

    def chunk(a, step):
        goal = (prim[a] + step) % RING
        parts = []
        for k in range(RING):
            side = (seco[a] + roles[k]) % RING
            parts.append(acts_c[goal * RING + side if a == 0 else side * RING + goal])
        return jnp.dot(g_t[pl.ds(a * half_cols, half_cols), :], jnp.concatenate(parts, axis=1),
                       preferred_element_type=F32)

    def cut(product, half, k):
        return product[half * 256:(half + 1) * 256, k * 128:(k + 1) * 128]

    def opp_copy(a, d):
        return pltpu.make_async_remote_copy(
            src_ref=s_opp.at[a, d], dst_ref=r_opp.at[a, d], send_sem=s1_opp.at[a, d],
            recv_sem=r1_opp.at[a, d], device_id=hop(a, d), device_id_type=MESH)

    def fin_copy(a, d, half, k):
        return pltpu.make_async_remote_copy(
            src_ref=s_nb.at[a, d, half, k], dst_ref=r_fin.at[a, d, half, k], send_sem=s1_fin.at[a, d, half, k],
            recv_sem=r1_fin.at[a, d, half, k], device_id=hop(a, d), device_id_type=MESH)

    def do_opp(a):
        product = chunk(a, 2)
        for d in (0, 1):
            for k in range(RING):
                s_opp[a, d, k] = cut(product, d, k).astype(BF16)
            opp_copy(a, d).start()

    def do_neighbour(a, d):
        product = chunk(a, 1 if d == 0 else 3)
        plain = 1 - d
        for k in range(RING):
            s_nb[a, d, plain, k] = cut(product, plain, k).astype(BF16)
            fin_copy(a, d, plain, k).start()
            hold[a, d, k] = cut(product, d, k)

    def do_pass(a, d):
        opp_copy(a, d).wait_recv()
        for k in range(RING):
            s_nb[a, d, d, k] = (hold[a, d, k] + r_opp[a, d, k].astype(F32)).astype(BF16)
            fin_copy(a, d, d, k).start()

    def do_own(a):
        product = chunk(a, 0)
        for half in (0, 1):
            for k in range(RING):
                own[a, half, k] = cut(product, half, k)

    for j in range(blocks):
        load_column(j).wait()
        send_column(j).wait_recv()
    scale(0)
    do_opp(0)
    scale(1)
    do_opp(1)
    do_neighbour(0, 0)
    do_neighbour(0, 1)
    do_neighbour(1, 0)
    do_pass(0, 0)
    do_pass(0, 1)
    do_neighbour(1, 1)
    do_pass(1, 0)
    do_pass(1, 1)
    do_own(0)
    do_own(1)

    def opp2_copy(a, d):
        return pltpu.make_async_remote_copy(
            src_ref=own.at[a, d, 0], dst_ref=r2_opp.at[a, d], send_sem=s2_opp.at[a, d],
            recv_sem=r2o_sem.at[a, d], device_id=hop(1 - a, d), device_id_type=MESH)

    def plain2_copy(a, d):
        return pltpu.make_async_remote_copy(
            src_ref=own.at[a, 1 - d, 1 + d], dst_ref=r2_fin.at[a, d, 1 - d], send_sem=s2_fin.at[a, d, 1 - d],
            recv_sem=r2f_sem.at[a, d, 1 - d], device_id=hop(1 - a, d), device_id_type=MESH)

    def pass2_copy(a, d):
        return pltpu.make_async_remote_copy(
            src_ref=s2.at[a, d], dst_ref=r2_fin.at[a, d, d], send_sem=s2_fin.at[a, d, d],
            recv_sem=r2f_sem.at[a, d, d], device_id=hop(1 - a, d), device_id_type=MESH)

    for k in range(RING):
        for a in (0, 1):
            for half in (0, 1):
                fin_copy(a, 0, half, k).wait_recv()
                fin_copy(a, 1, half, k).wait_recv()
                own[a, half, k] = own[a, half, k] + r_fin[a, 0, half, k].astype(F32) + r_fin[a, 1, half, k].astype(F32)
            if k == 0:
                opp2_copy(a, 0).start()
                opp2_copy(a, 1).start()
            elif k < 3:
                plain2_copy(a, k - 1).start()
    for a in (0, 1):
        for d in (0, 1):
            opp2_copy(a, d).wait_recv()
            s2[a, d] = own[a, d, 1 + d] + r2_opp[a, d]
            pass2_copy(a, d).start()
    for a in (0, 1):
        for half in (0, 1):
            for d in (0, 1):
                (pass2_copy if d == half else plain2_copy)(a, d).wait_recv()
            done = own[a, half, 3] + r2_fin[a, 0, half] + r2_fin[a, 1, half]
            out[:, pl.ds(a * half_cols + half * 256, 256)] = done.T

    send_grads.wait_send()
    for j in range(blocks):
        send_column(j).wait_send()
    for other, device in group:
        send_norms(other, device).wait_send()
    for a in (0, 1):
        for d in (0, 1):
            opp_copy(a, d).wait_send()
            for half in (0, 1):
                for k in range(RING):
                    fin_copy(a, d, half, k).wait_send()
            opp2_copy(a, d).wait_send()
            plain2_copy(a, d).wait_send()
            pass2_copy(a, d).wait_send()


def on_device(acts, out_grads, clip_bound, noise):
    tokens, width = acts.shape[1:]
    columns = out_grads.shape[2]
    rows = width // lax.axis_size("dp")
    examples = tokens // SEQ
    batch_total = examples * lax.axis_size("dp")
    out_factor = width / math.sqrt(batch_total)
    dma = pltpu.SemaphoreType.DMA
    summed = pl.pallas_call(
        kernel,
        out_shape=jax.ShapeDtypeStruct((rows, columns), F32),
        in_specs=[
            pl.BlockSpec(memory_space=pl.ANY),
            pl.BlockSpec(memory_space=pl.ANY),
            pl.BlockSpec(memory_space=pltpu.SMEM),
        ],
        out_specs=pl.BlockSpec(memory_space=pltpu.VMEM),
        scratch_shapes=[
            pltpu.VMEM((2, SEQ, width), BF16),
            pltpu.VMEM((2, tokens, columns), BF16),
            pltpu.VMEM((width // 256, 2 * tokens, 128), BF16),
            pltpu.VMEM((columns, 2 * tokens), BF16),
            pltpu.VMEM((examples, 8, 128), F32),
            pltpu.VMEM((8, examples, 8, 128), F32),
            pltpu.VMEM((2, 2, RING, 256, 128), BF16),
            pltpu.VMEM((2, 2, 2, RING, 256, 128), BF16),
            pltpu.VMEM((2, 2, RING, 256, 128), F32),
            pltpu.VMEM((2, 2, RING, 256, 128), BF16),
            pltpu.VMEM((2, 2, 2, RING, 256, 128), BF16),
            pltpu.VMEM((2, 2, RING, 256, 128), F32),
            pltpu.VMEM((2, 2, 256, 128), F32),
            pltpu.VMEM((2, 2, 256, 128), F32),
            pltpu.VMEM((2, 2, 2, 256, 128), F32),
            dma((2,)),
            dma((examples,)),
            dma((width // 256,)),
            dma((width // 256,)),
            dma((width // 256,)),
            dma,
            dma,
            dma((8,)),
            dma((8,)),
            dma((2, 2)),
            dma((2, 2)),
            dma((2, 2, 2, RING)),
            dma((2, 2, 2, RING)),
            dma((2, 2)),
            dma((2, 2)),
            dma((2, 2, 2)),
            dma((2, 2, 2)),
        ],
        compiler_params=pltpu.CompilerParams(
            collective_id=0, has_side_effects=True, vmem_limit_bytes=63 * 2**20
        ),
    )(acts[0], out_grads[0], clip_bound)
    return (summed * out_factor + noise[0])[None]


def solution(mesh):
    placed = (P(None, "dp", None), P(None, "dp", "mp"), P(), P(None, "dp", "mp"))
    return jax.shard_map(
        on_device, mesh=mesh, in_specs=placed, out_specs=P(None, "dp", "mp"), check_vma=False
    )
```

```python
import math

import jax
import jax.numpy as jnp
from jax import lax
from jax.experimental import pallas as pl
from jax.experimental.pallas import tpu as pltpu
from jax.sharding import PartitionSpec as P

SEQ = 512
RING = 4
MESH = pl.DeviceIdType.MESH
F32 = jnp.float32
BF16 = jnp.bfloat16
CONTRACT_LAST = (((1,), (1,)), ((), ()))


def fold(product):
    rows, cols = product.shape
    return jnp.sum(product.reshape(rows // 8, 8, cols // 128, 128), axis=(0, 2))


def kernel(acts, grads, bound, out, abuf, graw, acts_c, g_t, ahead, norm_own, norm_all,
           s_opp, s_nb, r_opp, r_fin, own, r2_opp, s2, r2_fin,
           abuf_sem, grad_sem, col_sem, xs_acts, xr_acts, xs_grads, xr_grads, ns_sem, nr_sem,
           s1_opp, r1_opp, s1_fin, r1_fin, s2_opp, r2o_sem, s2_fin, r2f_sem):
    dp = lax.axis_index("dp")
    y = lax.axis_index("mp")
    x, z, c = dp // (2 * RING), (dp // 2) % RING, dp % 2
    tokens = acts.shape[0]
    examples = tokens // SEQ
    blocks = acts.shape[1] // 256
    half_cols = grads.shape[1] // 2

    def at(xx, zz, cc=c, yy=y):
        return ((xx % RING) * (2 * RING) + (zz % RING) * 2 + cc, yy)

    partner = at(x, z, 1 - c)
    prim = (x, z)
    seco = (z, x)

    def hop(axis, direction):
        step = 1 if direction == 0 else RING - 1
        return at(x + step, z) if axis == 0 else at(x, z + step)

    roles = (2, 1, 3, 0)

    def load_acts(e, slot):
        return pltpu.make_async_copy(acts.at[pl.ds(e * SEQ, SEQ), :], abuf.at[slot], abuf_sem.at[slot])

    def load_grads(e):
        rows = pl.ds(e * SEQ, SEQ)
        return pltpu.make_async_copy(grads.at[rows, :], graw.at[c, rows, :], grad_sem.at[e])

    load_grads(0).start()
    load_acts(0, 0).start()

    peers = [hop(a, d) for a in (0, 1) for d in (0, 1)]
    me8 = c * 4 + y
    group = []
    for d in range(1, 8):
        other = (me8 + d) % 8
        group.append((other, at(x, z, other // 4, other % 4)))
    barrier = pltpu.get_barrier_semaphore()
    for device in peers + [g[1] for g in group]:
        pl.semaphore_signal(barrier, inc=1, device_id=device, device_id_type=MESH)
    mine = pl.ds(pl.multiple_of(c * tokens, tokens), tokens)
    send_grads = pltpu.make_async_remote_copy(
        src_ref=grads, dst_ref=graw.at[c], send_sem=xs_grads, recv_sem=xr_grads,
        device_id=partner, device_id_type=MESH)

    order = []
    for first in [(2, None), (None, 2), (1, None), (3, None), (None, 1), (None, 3), (0, None)]:
        for step in roles:
            pair = (first[0] if first[0] is not None else step, first[1] if first[1] is not None else step)
            if pair not in order:
                order.append(pair)

    def block(i):
        dx, dz = order[i]
        return ((x + dx) % RING) * RING + (z + dz) % RING

    def column_block(j, core):
        return pl.ds(pl.multiple_of(j * 256 + core * 128, 128), 128)

    def send_column(i):
        j = block(i)
        return pltpu.make_async_remote_copy(
            src_ref=acts.at[:, column_block(j, 1 - c)], dst_ref=acts_c.at[j, mine, :],
            send_sem=xs_acts.at[i], recv_sem=xr_acts.at[i], device_id=partner, device_id_type=MESH)

    def load_column(i):
        j = block(i)
        return pltpu.make_async_copy(acts.at[:, column_block(j, c)], acts_c.at[j, mine, :], col_sem.at[i])

    def do_gram(e):
        slot = e % 2
        load_grads(e).wait()
        load_acts(e, slot).wait()
        if e + 1 < examples:
            load_grads(e + 1).start()
        if e == 0:
            load_acts(1, 1).start()
        b_all = graw[c, pl.ds(e * SEQ, SEQ), :]
        b_low = graw[c, pl.ds(e * SEQ, 256), :]
        b_high = graw[c, pl.ds(e * SEQ + 256, 256), :]
        ga = lax.dot_general(abuf[slot], abuf[slot, pl.ds(0, 256), :], CONTRACT_LAST, preferred_element_type=F32)
        gb = lax.dot_general(b_all, b_low, CONTRACT_LAST, preferred_element_type=F32)
        both = ga * gb
        total = fold(both[:256]) + 2.0 * fold(both[256:])
        a_high = abuf[slot, pl.ds(256, 256), :]
        ga = lax.dot_general(a_high, a_high, CONTRACT_LAST, preferred_element_type=F32)
        gb = lax.dot_general(b_high, b_high, CONTRACT_LAST, preferred_element_type=F32)
        norm_own[e] = total + fold(ga * gb)
        if e + 2 < examples:
            load_acts(e + 2, slot).start()
        columns = pl.ds(pl.multiple_of(c * tokens + e * SEQ, SEQ), SEQ)
        g_t[:, columns] = b_all.T

    early = 4
    do_gram(0)
    pl.semaphore_wait(barrier, 11)
    send_grads.start()
    for i in range(early):
        send_column(i).start()
    for e in range(1, examples):
        do_gram(e)
        for i in range((e - 1) * 4, blocks if e + 1 == examples else e * 4):
            load_column(i).start()

    def send_norms(other, device):
        return pltpu.make_async_remote_copy(
            src_ref=norm_own, dst_ref=norm_all.at[me8], send_sem=ns_sem.at[other],
            recv_sem=nr_sem.at[me8], device_id=device, device_id_type=MESH)

    for other, device in group:
        send_norms(other, device).start()
    for i in range(early, blocks):
        send_column(i).start()

    def do_theirs():
        send_grads.wait_recv()
        theirs = 1 - c
        for e in range(examples):
            columns = pl.ds(pl.multiple_of(theirs * tokens + e * SEQ, SEQ), SEQ)
            g_t[:, columns] = graw[theirs, pl.ds(e * SEQ, SEQ), :].T

    do_theirs()

    arrived = set()

    def chunk_blocks(a, step):
        indices = [order.index((step, role) if a == 0 else (role, step)) for role in roles]
        for i in indices:
            if i not in arrived:
                arrived.add(i)
                load_column(i).wait()
                send_column(i).wait_recv()
        return [block(i) for i in indices]

    def chunk(a, step, half):
        right = jnp.concatenate([acts_c[j] for j in chunk_blocks(a, step)], axis=1)
        return jnp.dot(g_t[pl.ds(a * half_cols + half * 256, 256), :], right, preferred_element_type=F32)

    def cut(product, k):
        return product[:, k * 128:(k + 1) * 128]

    def do_ahead(half):
        places = chunk_blocks(0, 2)
        for e in range(2 * examples):
            span = pl.ds(e * SEQ, SEQ)
            right = jnp.concatenate([acts_c[j, span, :] for j in places], axis=1)
            ahead[half, e] = jnp.dot(g_t[pl.ds(half * 256, 256), span], right, preferred_element_type=F32)

    do_ahead(0)
    do_ahead(1)

    def do_norm_wait():
        norm_all[me8] = norm_own[...]
        for other, device in group:
            pltpu.make_async_remote_copy(
                src_ref=norm_own, dst_ref=norm_all.at[other], send_sem=ns_sem.at[other],
                recv_sem=nr_sem.at[other], device_id=device, device_id_type=MESH).wait_recv()

    do_norm_wait()

    limit = bound[0]
    factors = []
    for core in range(2):
        summed = norm_all[4 * core] + norm_all[4 * core + 1] + norm_all[4 * core + 2] + norm_all[4 * core + 3]
        for e in range(examples):
            norm_sq = jnp.sum(summed[e], axis=(0, 1), keepdims=True)
            clip = jnp.minimum(1.0, limit / jnp.sqrt(norm_sq + 1e-06))
            factors.append(clip / limit)

    def do_scale(a, half):
        for e, factor in enumerate(factors):
            rows, columns = pl.ds(a * half_cols + half * 256, 256), pl.ds(e * SEQ, SEQ)
            g_t[rows, columns] = (g_t[rows, columns].astype(F32) * factor).astype(BF16)

    def opp_copy(a, d):
        return pltpu.make_async_remote_copy(
            src_ref=s_opp.at[a, d], dst_ref=r_opp.at[a, d], send_sem=s1_opp.at[a, d],
            recv_sem=r1_opp.at[a, d], device_id=hop(a, d), device_id_type=MESH)

    def fin_copy(a, d, half, k):
        return pltpu.make_async_remote_copy(
            src_ref=s_nb.at[a, d, half, k], dst_ref=r_fin.at[a, d, half, k], send_sem=s1_fin.at[a, d, half, k],
            recv_sem=r1_fin.at[a, d, half, k], device_id=hop(a, d), device_id_type=MESH)

    def do_opp(a, d):
        if a == 0:
            product = ahead[d, 0] * factors[0]
            for e in range(1, 2 * examples):
                product = product + ahead[d, e] * factors[e]
        else:
            product = chunk(a, 2, d)
        for k in range(RING):
            s_opp[a, d, k] = cut(product, k).astype(BF16)
        opp_copy(a, d).start()

    def do_plain(a, d):
        product = chunk(a, 1 if d == 0 else 3, 1 - d)
        for k in range(RING):
            s_nb[a, d, 1 - d, k] = cut(product, k).astype(BF16)
            fin_copy(a, d, 1 - d, k).start()

    def do_pass(a, d):
        product = chunk(a, 1 if d == 0 else 3, d)
        opp_copy(a, d).wait_recv()
        for k in range(RING):
            s_nb[a, d, d, k] = (cut(product, k) + r_opp[a, d, k].astype(F32)).astype(BF16)
            fin_copy(a, d, d, k).start()

    def do_own(a, half):
        product = chunk(a, 0, half)
        for k in range(RING):
            own[a, half, k] = cut(product, k)

    pairs = [(a, d) for a in (0, 1) for d in (0, 1)]
    do_opp(0, 0)
    do_opp(0, 1)
    for d in (0, 1):
        do_scale(1, d)
        do_opp(1, d)
    for a, d in pairs:
        if a == 0:
            do_scale(0, 1 - d)
        do_plain(a, d)
    for a, d in pairs:
        do_pass(a, d)
    do_own(0, 0)
    do_own(0, 1)

    def opp2_copy(a, d):
        return pltpu.make_async_remote_copy(
            src_ref=own.at[a, d, 0], dst_ref=r2_opp.at[a, d], send_sem=s2_opp.at[a, d],
            recv_sem=r2o_sem.at[a, d], device_id=hop(1 - a, d), device_id_type=MESH)

    def plain2_copy(a, d):
        return pltpu.make_async_remote_copy(
            src_ref=own.at[a, 1 - d, 1 + d], dst_ref=r2_fin.at[a, d, 1 - d], send_sem=s2_fin.at[a, d, 1 - d],
            recv_sem=r2f_sem.at[a, d, 1 - d], device_id=hop(1 - a, d), device_id_type=MESH)

    def pass2_copy(a, d):
        return pltpu.make_async_remote_copy(
            src_ref=s2.at[a, d], dst_ref=r2_fin.at[a, d, d], send_sem=s2_fin.at[a, d, d],
            recv_sem=r2f_sem.at[a, d, d], device_id=hop(1 - a, d), device_id_type=MESH)

    def do_join(a, k):
        for half in (0, 1):
            fin_copy(a, 0, half, k).wait_recv()
            fin_copy(a, 1, half, k).wait_recv()
            own[a, half, k] = own[a, half, k] + r_fin[a, 0, half, k].astype(F32) + r_fin[a, 1, half, k].astype(F32)
        if k == 0:
            opp2_copy(a, 0).start()
            opp2_copy(a, 1).start()
        elif k < 3:
            plain2_copy(a, k - 1).start()

    def do_pass2(a, d):
        opp2_copy(a, d).wait_recv()
        s2[a, d] = own[a, d, 1 + d] + r2_opp[a, d]
        pass2_copy(a, d).start()

    def do_finish(a, half):
        for d in (0, 1):
            (pass2_copy if d == half else plain2_copy)(a, d).wait_recv()
        done = own[a, half, 3] + r2_fin[a, 0, half] + r2_fin[a, 1, half]
        out[:, pl.ds(a * half_cols + half * 256, 256)] = done.T

    do_join(0, 0)
    do_own(1, 0)
    do_own(1, 1)
    do_join(1, 0)
    for k in range(1, RING):
        do_join(0, k)
        do_join(1, k)
    for a in (0, 1):
        for d in (0, 1):
            do_pass2(a, d)
    for a in (0, 1):
        for half in (0, 1):
            do_finish(a, half)

    send_grads.wait_send()
    for i in range(blocks):
        send_column(i).wait_send()
    for other, device in group:
        send_norms(other, device).wait_send()
    for a in (0, 1):
        for d in (0, 1):
            opp_copy(a, d).wait_send()
            for half in (0, 1):
                for k in range(RING):
                    fin_copy(a, d, half, k).wait_send()
            opp2_copy(a, d).wait_send()
            plain2_copy(a, d).wait_send()
            pass2_copy(a, d).wait_send()


def on_device(acts, out_grads, clip_bound, noise):
    tokens, width = acts.shape[1:]
    columns = out_grads.shape[2]
    rows = width // lax.axis_size("dp")
    examples = tokens // SEQ
    batch_total = examples * lax.axis_size("dp")
    out_factor = width / math.sqrt(batch_total)
    dma = pltpu.SemaphoreType.DMA
    summed = pl.pallas_call(
        kernel,
        out_shape=jax.ShapeDtypeStruct((rows, columns), F32),
        in_specs=[
            pl.BlockSpec(memory_space=pl.ANY),
            pl.BlockSpec(memory_space=pl.ANY),
            pl.BlockSpec(memory_space=pltpu.SMEM),
        ],
        out_specs=pl.BlockSpec(memory_space=pltpu.VMEM),
        scratch_shapes=[
            pltpu.VMEM((2, SEQ, width), BF16),
            pltpu.VMEM((2, tokens, columns), BF16),
            pltpu.VMEM((width // 256, 2 * tokens, 128), BF16),
            pltpu.VMEM((columns, 2 * tokens), BF16),
            pltpu.VMEM((2, 2 * examples, 256, RING * 128), F32),
            pltpu.VMEM((examples, 8, 128), F32),
            pltpu.VMEM((8, examples, 8, 128), F32),
            pltpu.VMEM((2, 2, RING, 256, 128), BF16),
            pltpu.VMEM((2, 2, 2, RING, 256, 128), BF16),
            pltpu.VMEM((2, 2, RING, 256, 128), BF16),
            pltpu.VMEM((2, 2, 2, RING, 256, 128), BF16),
            pltpu.VMEM((2, 2, RING, 256, 128), F32),
            pltpu.VMEM((2, 2, 256, 128), F32),
            pltpu.VMEM((2, 2, 256, 128), F32),
            pltpu.VMEM((2, 2, 2, 256, 128), F32),
            dma((2,)),
            dma((examples,)),
            dma((width // 256,)),
            dma((width // 256,)),
            dma((width // 256,)),
            dma,
            dma,
            dma((8,)),
            dma((8,)),
            dma((2, 2)),
            dma((2, 2)),
            dma((2, 2, 2, RING)),
            dma((2, 2, 2, RING)),
            dma((2, 2)),
            dma((2, 2)),
            dma((2, 2, 2)),
            dma((2, 2, 2)),
        ],
        compiler_params=pltpu.CompilerParams(
            collective_id=0, has_side_effects=True, vmem_limit_bytes=63 * 2**20
        ),
    )(acts[0], out_grads[0], clip_bound)
    return (summed * out_factor + noise[0])[None]


def solution(mesh):
    placed = (P(None, "dp", None), P(None, "dp", "mp"), P(), P(None, "dp", "mp"))
    return jax.shard_map(
        on_device, mesh=mesh, in_specs=placed, out_specs=P(None, "dp", "mp"), check_vma=False
    )
```

```python
import math

import jax
import jax.numpy as jnp
from jax import lax
from jax.experimental import pallas as pl
from jax.experimental.pallas import tpu as pltpu
from jax.sharding import PartitionSpec as P

SEQ = 512
RING = 4
MESH = pl.DeviceIdType.MESH
F32 = jnp.float32
BF16 = jnp.bfloat16
CONTRACT_LAST = (((1,), (1,)), ((), ()))


def fold(product):
    rows, cols = product.shape
    return jnp.sum(product.reshape(rows // 8, 8, cols // 128, 128), axis=(0, 2))


def kernel(acts, grads, bound, out, abuf, graw, acts_c, g_t, ahead, norm_own, norm_all,
           s_opp, s_nb, r_opp, r_fin, own, r2_opp, s2, r2_fin,
           abuf_sem, grad_sem, col_sem, xs_acts, xr_acts, xs_grads, xr_grads, ns_sem, nr_sem,
           s1_opp, r1_opp, s1_fin, r1_fin, s2_opp, r2o_sem, s2_fin, r2f_sem):
    dp = lax.axis_index("dp")
    y = lax.axis_index("mp")
    x, z, c = dp // (2 * RING), (dp // 2) % RING, dp % 2
    tokens = acts.shape[0]
    examples = tokens // SEQ
    blocks = acts.shape[1] // 256
    half_cols = grads.shape[1] // 2

    def at(xx, zz, cc=c, yy=y):
        return ((xx % RING) * (2 * RING) + (zz % RING) * 2 + cc, yy)

    partner = at(x, z, 1 - c)

    def swapped(core, u, v):
        return u + core * (v - u), v + core * (u - v)

    def hop(axis, direction):
        step = 1 if direction == 0 else RING - 1
        dx, dz = swapped(c, step, 0) if axis == 0 else swapped(c, 0, step)
        return at(x + dx, z + dz)

    roles = (2, 1, 3, 0)

    def load_acts(e, slot):
        return pltpu.make_async_copy(acts.at[pl.ds(e * SEQ, SEQ), :], abuf.at[slot], abuf_sem.at[slot])

    def load_grads(e):
        rows = pl.ds(e * SEQ, SEQ)
        return pltpu.make_async_copy(grads.at[rows, :], graw.at[c, rows, :], grad_sem.at[e])

    load_grads(0).start()
    load_acts(0, 0).start()

    peers = [hop(a, d) for a in (0, 1) for d in (0, 1)]
    me8 = c * 4 + y
    group = []
    for d in range(1, 8):
        other = (me8 + d) % 8
        group.append((other, at(x, z, other // 4, other % 4)))
    barrier = pltpu.get_barrier_semaphore()
    for device in peers + [g[1] for g in group]:
        pl.semaphore_signal(barrier, inc=1, device_id=device, device_id_type=MESH)
    mine = pl.ds(pl.multiple_of(c * tokens, tokens), tokens)
    send_grads = pltpu.make_async_remote_copy(
        src_ref=grads, dst_ref=graw.at[c], send_sem=xs_grads, recv_sem=xr_grads,
        device_id=partner, device_id_type=MESH)

    order = []
    for first in [(2, None), (None, 2), (1, None), (3, None), (None, 1), (None, 3), (0, None)]:
        for step in roles:
            pair = (first[0] if first[0] is not None else step, first[1] if first[1] is not None else step)
            if pair not in order:
                order.append(pair)

    def block(i, core):
        dx, dz = swapped(core, *order[i])
        return ((x + dx) % RING) * RING + (z + dz) % RING

    def column_block(j, core):
        return pl.ds(pl.multiple_of(j * 256 + core * 128, 128), 128)

    def send_column(i):
        j = block(i, 1 - c)
        return pltpu.make_async_remote_copy(
            src_ref=acts.at[:, column_block(j, 1 - c)], dst_ref=acts_c.at[j, mine, :],
            send_sem=xs_acts.at[i], recv_sem=xr_acts.at[i], device_id=partner, device_id_type=MESH)

    def load_column(i):
        j = block(i, c)
        return pltpu.make_async_copy(acts.at[:, column_block(j, c)], acts_c.at[j, mine, :], col_sem.at[i])

    def do_gram(e):
        slot = e % 2
        load_grads(e).wait()
        load_acts(e, slot).wait()
        if e + 1 < examples:
            load_grads(e + 1).start()
        if e == 0:
            load_acts(1, 1).start()
        b_all = graw[c, pl.ds(e * SEQ, SEQ), :]
        b_low = graw[c, pl.ds(e * SEQ, 256), :]
        b_high = graw[c, pl.ds(e * SEQ + 256, 256), :]
        ga = lax.dot_general(abuf[slot], abuf[slot, pl.ds(0, 256), :], CONTRACT_LAST, preferred_element_type=F32)
        gb = lax.dot_general(b_all, b_low, CONTRACT_LAST, preferred_element_type=F32)
        both = ga * gb
        total = fold(both[:256]) + 2.0 * fold(both[256:])
        a_high = abuf[slot, pl.ds(256, 256), :]
        ga = lax.dot_general(a_high, a_high, CONTRACT_LAST, preferred_element_type=F32)
        gb = lax.dot_general(b_high, b_high, CONTRACT_LAST, preferred_element_type=F32)
        norm_own[e] = total + fold(ga * gb)
        if e + 2 < examples:
            load_acts(e + 2, slot).start()
        columns = pl.ds(pl.multiple_of(c * tokens + e * SEQ, SEQ), SEQ)
        g_t[:, columns] = b_all.T

    early = 4
    do_gram(0)
    pl.semaphore_wait(barrier, 11)
    send_grads.start()
    for i in range(early):
        send_column(i).start()
    for e in range(1, examples):
        do_gram(e)
        for i in range((e - 1) * 4, blocks if e + 1 == examples else e * 4):
            load_column(i).start()

    def send_norms(other, device):
        return pltpu.make_async_remote_copy(
            src_ref=norm_own, dst_ref=norm_all.at[me8], send_sem=ns_sem.at[other],
            recv_sem=nr_sem.at[me8], device_id=device, device_id_type=MESH)

    for other, device in group:
        send_norms(other, device).start()
    for i in range(early, blocks):
        send_column(i).start()

    def do_theirs():
        send_grads.wait_recv()
        theirs = 1 - c
        for e in range(examples):
            columns = pl.ds(pl.multiple_of(theirs * tokens + e * SEQ, SEQ), SEQ)
            g_t[:, columns] = graw[theirs, pl.ds(e * SEQ, SEQ), :].T

    do_theirs()

    arrived = set()

    def chunk_blocks(a, step):
        indices = [order.index((step, role) if a == 0 else (role, step)) for role in roles]
        for i in indices:
            if i not in arrived:
                arrived.add(i)
                load_column(i).wait()
                send_column(i).wait_recv()
        return [block(i, c) for i in indices]

    def chunk(a, step, half):
        right = jnp.concatenate([acts_c[j] for j in chunk_blocks(a, step)], axis=1)
        return jnp.dot(g_t[pl.ds(a * half_cols + half * 256, 256), :], right, preferred_element_type=F32)

    def cut(product, k):
        return product[:, k * 128:(k + 1) * 128]

    def do_ahead(half):
        places = chunk_blocks(0, 2)
        for e in range(2 * examples):
            span = pl.ds(e * SEQ, SEQ)
            right = jnp.concatenate([acts_c[j, span, :] for j in places], axis=1)
            ahead[half, e] = jnp.dot(g_t[pl.ds(half * 256, 256), span], right, preferred_element_type=F32)

    do_ahead(0)
    do_ahead(1)

    def do_norm_wait():
        norm_all[me8] = norm_own[...]
        for other, device in group:
            pltpu.make_async_remote_copy(
                src_ref=norm_own, dst_ref=norm_all.at[other], send_sem=ns_sem.at[other],
                recv_sem=nr_sem.at[other], device_id=device, device_id_type=MESH).wait_recv()

    do_norm_wait()

    limit = bound[0]
    factors = []
    for core in range(2):
        summed = norm_all[4 * core] + norm_all[4 * core + 1] + norm_all[4 * core + 2] + norm_all[4 * core + 3]
        for e in range(examples):
            norm_sq = jnp.sum(summed[e], axis=(0, 1), keepdims=True)
            clip = jnp.minimum(1.0, limit / jnp.sqrt(norm_sq + 1e-06))
            factors.append(clip / limit)

    def do_scale(a, half):
        for e, factor in enumerate(factors):
            rows, columns = pl.ds(a * half_cols + half * 256, 256), pl.ds(e * SEQ, SEQ)
            g_t[rows, columns] = (g_t[rows, columns].astype(F32) * factor).astype(BF16)

    def opp_copy(a, d):
        return pltpu.make_async_remote_copy(
            src_ref=s_opp.at[a, d], dst_ref=r_opp.at[a, d], send_sem=s1_opp.at[a, d],
            recv_sem=r1_opp.at[a, d], device_id=hop(a, d), device_id_type=MESH)

    def fin_copy(a, d, half, k):
        return pltpu.make_async_remote_copy(
            src_ref=s_nb.at[a, d, half, k], dst_ref=r_fin.at[a, d, half, k], send_sem=s1_fin.at[a, d, half, k],
            recv_sem=r1_fin.at[a, d, half, k], device_id=hop(a, d), device_id_type=MESH)

    def do_opp(a, d):
        if a == 0:
            product = ahead[d, 0] * factors[0]
            for e in range(1, 2 * examples):
                product = product + ahead[d, e] * factors[e]
        else:
            product = chunk(a, 2, d)
        for k in range(RING):
            s_opp[a, d, k] = cut(product, k).astype(BF16)
        opp_copy(a, d).start()

    def do_plain(a, d):
        product = chunk(a, 1 if d == 0 else 3, 1 - d)
        for k in range(RING):
            s_nb[a, d, 1 - d, k] = cut(product, k).astype(BF16)
            fin_copy(a, d, 1 - d, k).start()

    def do_pass(a, d):
        product = chunk(a, 1 if d == 0 else 3, d)
        opp_copy(a, d).wait_recv()
        for k in range(RING):
            s_nb[a, d, d, k] = (cut(product, k) + r_opp[a, d, k].astype(F32)).astype(BF16)
            fin_copy(a, d, d, k).start()

    def do_own(a, half):
        product = chunk(a, 0, half)
        for k in range(RING):
            own[a, half, k] = cut(product, k)

    pairs = [(a, d) for a in (0, 1) for d in (0, 1)]
    do_opp(0, 0)
    do_opp(0, 1)
    for d in (0, 1):
        do_scale(1, d)
        do_opp(1, d)
    for a, d in pairs:
        if a == 0:
            do_scale(0, 1 - d)
        do_plain(a, d)
    for a, d in pairs:
        do_pass(a, d)
    do_own(0, 0)
    do_own(0, 1)

    def opp2_copy(a, d):
        return pltpu.make_async_remote_copy(
            src_ref=own.at[a, d, 0], dst_ref=r2_opp.at[a, d], send_sem=s2_opp.at[a, d],
            recv_sem=r2o_sem.at[a, d], device_id=hop(1 - a, d), device_id_type=MESH)

    def plain2_copy(a, d):
        return pltpu.make_async_remote_copy(
            src_ref=own.at[a, 1 - d, 1 + d], dst_ref=r2_fin.at[a, d, 1 - d], send_sem=s2_fin.at[a, d, 1 - d],
            recv_sem=r2f_sem.at[a, d, 1 - d], device_id=hop(1 - a, d), device_id_type=MESH)

    def pass2_copy(a, d):
        return pltpu.make_async_remote_copy(
            src_ref=s2.at[a, d], dst_ref=r2_fin.at[a, d, d], send_sem=s2_fin.at[a, d, d],
            recv_sem=r2f_sem.at[a, d, d], device_id=hop(1 - a, d), device_id_type=MESH)

    def do_join(a, k):
        for half in (0, 1):
            fin_copy(a, 0, half, k).wait_recv()
            fin_copy(a, 1, half, k).wait_recv()
            own[a, half, k] = own[a, half, k] + r_fin[a, 0, half, k].astype(F32) + r_fin[a, 1, half, k].astype(F32)
        if k == 0:
            opp2_copy(a, 0).start()
            opp2_copy(a, 1).start()
        elif k < 3:
            plain2_copy(a, k - 1).start()

    def do_pass2(a, d):
        opp2_copy(a, d).wait_recv()
        s2[a, d] = own[a, d, 1 + d] + r2_opp[a, d]
        pass2_copy(a, d).start()

    def do_finish(a, half):
        for d in (0, 1):
            (pass2_copy if d == half else plain2_copy)(a, d).wait_recv()
        done = own[a, half, 3] + r2_fin[a, 0, half] + r2_fin[a, 1, half]
        out[:, pl.ds(a * half_cols + half * 256, 256)] = done.T

    do_join(0, 0)
    do_own(1, 0)
    do_own(1, 1)
    do_join(1, 0)
    for k in range(1, RING):
        do_join(0, k)
        do_join(1, k)
    for a in (0, 1):
        for d in (0, 1):
            do_pass2(a, d)
    for a in (0, 1):
        for half in (0, 1):
            do_finish(a, half)

    send_grads.wait_send()
    for i in range(blocks):
        send_column(i).wait_send()
    for other, device in group:
        send_norms(other, device).wait_send()
    for a in (0, 1):
        for d in (0, 1):
            opp_copy(a, d).wait_send()
            for half in (0, 1):
                for k in range(RING):
                    fin_copy(a, d, half, k).wait_send()
            opp2_copy(a, d).wait_send()
            plain2_copy(a, d).wait_send()
            pass2_copy(a, d).wait_send()


def on_device(acts, out_grads, clip_bound, noise):
    tokens, width = acts.shape[1:]
    columns = out_grads.shape[2]
    rows = width // lax.axis_size("dp")
    examples = tokens // SEQ
    batch_total = examples * lax.axis_size("dp")
    out_factor = width / math.sqrt(batch_total)
    dma = pltpu.SemaphoreType.DMA
    summed = pl.pallas_call(
        kernel,
        out_shape=jax.ShapeDtypeStruct((rows, columns), F32),
        in_specs=[
            pl.BlockSpec(memory_space=pl.ANY),
            pl.BlockSpec(memory_space=pl.ANY),
            pl.BlockSpec(memory_space=pltpu.SMEM),
        ],
        out_specs=pl.BlockSpec(memory_space=pltpu.VMEM),
        scratch_shapes=[
            pltpu.VMEM((2, SEQ, width), BF16),
            pltpu.VMEM((2, tokens, columns), BF16),
            pltpu.VMEM((width // 256, 2 * tokens, 128), BF16),
            pltpu.VMEM((columns, 2 * tokens), BF16),
            pltpu.VMEM((2, 2 * examples, 256, RING * 128), F32),
            pltpu.VMEM((examples, 8, 128), F32),
            pltpu.VMEM((8, examples, 8, 128), F32),
            pltpu.VMEM((2, 2, RING, 256, 128), BF16),
            pltpu.VMEM((2, 2, 2, RING, 256, 128), BF16),
            pltpu.VMEM((2, 2, RING, 256, 128), BF16),
            pltpu.VMEM((2, 2, 2, RING, 256, 128), BF16),
            pltpu.VMEM((2, 2, RING, 256, 128), F32),
            pltpu.VMEM((2, 2, 256, 128), F32),
            pltpu.VMEM((2, 2, 256, 128), F32),
            pltpu.VMEM((2, 2, 2, 256, 128), F32),
            dma((2,)),
            dma((examples,)),
            dma((width // 256,)),
            dma((width // 256,)),
            dma((width // 256,)),
            dma,
            dma,
            dma((8,)),
            dma((8,)),
            dma((2, 2)),
            dma((2, 2)),
            dma((2, 2, 2, RING)),
            dma((2, 2, 2, RING)),
            dma((2, 2)),
            dma((2, 2)),
            dma((2, 2, 2)),
            dma((2, 2, 2)),
        ],
        compiler_params=pltpu.CompilerParams(
            collective_id=0, has_side_effects=True, vmem_limit_bytes=63 * 2**20
        ),
    )(acts[0], out_grads[0], clip_bound)
    return (summed * out_factor + noise[0])[None]


def solution(mesh):
    placed = (P(None, "dp", None), P(None, "dp", "mp"), P(), P(None, "dp", "mp"))
    return jax.shard_map(
        on_device, mesh=mesh, in_specs=placed, out_specs=P(None, "dp", "mp"), check_vma=False
    )
```
